32 devices in a mesh: rng: 2 (over x), az: 16 (over z, y, core).
Axes of the slice: x: 2, y: 2, z: 4, core: 2. Of those that a mesh axis runs over, the one named last changes fastest.
Arguments:
- spectrum: float32 [1024, 2, 32768], P('rng', None, 'az'), may hold values from -9 to 9
- src_block: int32 [256, 8], P('az', 'rng'), may hold values from 0 to 6, as said below
- offsets: int32 [256, 1024], P('az', 'rng'), may hold values from 0 to 127
- tap_weights: float32 [8, 256, 1024], P(None, 'az', 'rng'), may hold values from -2 to 2
Outputs:
- image: float32 [1024, 2, 32768], P(('rng', 'az'))
The draws below stay inside these ranges and needn't reach their ends.
Inputs may be any that keep to these rules, and one draw needn't show every extreme that they name: src_block[g, b] lies between min(b, 6) and min(b + 5, 6); a shift of 5 blocks occurs in every draw.
All inputs are finite; a program needn't handle non-finite values.
Results may differ from the reference program's by a relative error of at most 0.00007.
Values sent between devices are 32-bit elements; how exact they have to be, the bound alone decides.
A program may use at most 192 MiB of HBM per device.

```python
import jax
import jax.numpy as jnp
from jax import lax

NA = 32768
NRB = 1024
BLOCK = 128
GW = 128
TAPS = 8
SHIFT_B = 5
NG = 256
NOB = 8


def draw_spectrum(key, part):
    position = jnp.arange(NRB, dtype=jnp.float32) / NRB
    noise = jnp.clip(jax.random.normal(key, (NRB, 2, NA), jnp.float32), -5.0, 5.0)
    amplitude = jnp.sqrt(1.0 + 2.0 * position)
    return noise * amplitude[:, None, None]


def draw_src_block(key, part):
    groups = jnp.arange(NG, dtype=jnp.int32)
    blocks = jnp.arange(NOB, dtype=jnp.int32)
    distance = jnp.abs(2 * groups + 1 - NG)
    baseline = SHIFT_B * distance // NG
    jitter = jax.random.randint(key, (NG, NOB), 0, 2).astype(jnp.int32)
    shifted = jnp.minimum(baseline[:, None] + jitter, SHIFT_B)
    shifted = jnp.where(groups[:, None] == 0, SHIFT_B, shifted)
    return jnp.minimum(blocks[None, :] + shifted, NOB - 2).astype(jnp.int32)


def place_ends(result, rng, smallest, largest):
    index_at = [jax.random.randint(jax.random.fold_in(rng, axis), (), 0, length) for axis, length in enumerate(result.shape)]
    widest = result.shape.index(max(result.shape))
    beside = index_at[:widest] + [(index_at[widest] + 1) % result.shape[widest]] + index_at[widest + 1:]
    return result.at[tuple(index_at)].set(smallest).at[tuple(beside)].set(largest)


def block_levels(key, shape, shards, smallest, high):
    loudness, own = 1.0, jax.random.fold_in(key, 6)
    for axis_at, parts in shards:
        heights = jnp.exp(jax.random.uniform(jax.random.fold_in(own, axis_at), (parts,), jnp.float32, smallest / len(shards), high / len(shards)))
        loudness = loudness * jnp.repeat(heights, shape[axis_at] // parts).reshape([-1 if axis == axis_at else 1 for axis in range(len(shape))])
    return loudness


def scatter_about(stream_key, dims, spread, reach, split=(), held_as=jnp.bfloat16):
    level = block_levels(stream_key, dims, split, -0.22, 0.18) if split else 1.0
    entries = jax.random.normal(stream_key, dims, jnp.float32) * spread * level
    return jnp.minimum(jnp.maximum(entries, -reach), reach).astype(held_as)


def setup_inputs(seed: int = 0) -> dict:
    keys = jax.random.split(jax.random.key(seed), 5)
    spectrum = draw_spectrum(jax.random.fold_in(keys[4], 71), 0)
    src_block = draw_src_block(jax.random.fold_in(keys[4], 71), 0)
    offsets = place_ends(jax.random.randint(keys[2], (NG, NRB), 0, BLOCK), jax.random.fold_in(keys[2], 1), 0, BLOCK - 1).astype(jnp.int32)
    tap_weights = scatter_about(keys[3], (TAPS, NG, NRB), 0.35, 2.0, ((1, 16), (2, 2)), jnp.float32)
    return dict(spectrum=spectrum, src_block=src_block, offsets=offsets, tap_weights=tap_weights)


def reference(spectrum, src_block, offsets, tap_weights):
    grouped = spectrum.reshape(NRB, 2, NG, GW).transpose(2, 0, 1, 3).reshape(NG, NRB, 2 * GW)
    src_rows = (src_block[:, :, None] * BLOCK + offsets.reshape(NG, NOB, BLOCK)).reshape(NG, NRB).astype(jnp.int32)

    def pick(table, where):
        return jnp.take(table, where, axis=0)
    remapped = jnp.zeros((NG, NRB, 2 * GW), jnp.float32)
    for tap_index in range(TAPS):
        picked = jax.vmap(pick)(grouped, src_rows + tap_index)
        remapped = remapped + tap_weights[tap_index][:, :, None] * picked
    remapped = remapped.reshape(NG, NRB, 2, GW).transpose(1, 2, 0, 3).reshape(NRB, 2, NA)
    values = jnp.fft.ifft(remapped[:, 0] + 1j * remapped[:, 1], axis=-1)
    band = jnp.stack([jnp.real(values), jnp.imag(values)], axis=1).astype(jnp.float32)
    energy = jnp.sum(band * band)
    scaling = lax.rsqrt(energy / (NRB * NA) + 1e-06)
    return band * scaling
```

```python
import functools
import math

import jax
import jax.numpy as jnp
import numpy as np
from jax import lax
from jax.experimental import pallas as pl
from jax.experimental.pallas import tpu as pltpu
from jax.sharding import PartitionSpec as P

BLOCK = 128
GW = 128
TAPS = 8
SHIFT_B = 5
WINDOW = 144
CHUNK_GROUPS = 4


def split_np(x):
    hi = x.astype(jnp.bfloat16)
    lo = (x - hi.astype(np.float64)).astype(jnp.bfloat16)
    return hi, lo


def split(x):
    hi = x.astype(jnp.bfloat16)
    lo = (x - hi.astype(jnp.float32)).astype(jnp.bfloat16)
    return hi, lo


def dft_tables(az_count, groups, per_chunk):
    total_groups = az_count * groups
    chunks = groups // per_chunk
    total_len = total_groups * GW
    k1 = np.arange(total_groups)
    ch, az, gl = np.meshgrid(np.arange(chunks), np.arange(az_count), np.arange(per_chunk), indexing="ij")
    g = (az * groups + ch * per_chunk + gl).reshape(-1)
    angle = 2.0 * np.pi * ((k1[:, None] * g[None, :]) % total_groups) / total_groups
    first = np.empty((2, total_groups, g.size, 2))
    first[0, :, :, 0] = np.cos(angle)
    first[0, :, :, 1] = -np.sin(angle)
    first[1, :, :, 0] = np.sin(angle)
    first[1, :, :, 1] = np.cos(angle)
    first = first.reshape(2 * total_groups, 2 * total_groups)
    l = np.arange(GW)
    turn = 2.0 * np.pi * (k1[:, None] * l[None, :]) / total_len
    twist = np.stack([np.cos(turn), np.sin(turn)]).astype(np.float32) / np.float32(total_len)
    inner = 2.0 * np.pi * ((l[:, None] * l[None, :]) % GW) / GW
    second = np.empty((2, GW, 2, GW))
    second[0, :, 0] = np.cos(inner)
    second[0, :, 1] = -np.sin(inner)
    second[1, :, 0] = np.sin(inner)
    second[1, :, 1] = np.cos(inner)
    second = second.reshape(2 * GW, 2 * GW)
    a_hi, a_lo = split_np(first)
    b_hi, b_lo = split_np(second)
    return a_hi, a_lo, twist, b_hi, b_lo


def remap_group(ext, out, sub, gl, blocks, src_of, off_row, weight_row):
    energy = jnp.zeros((8, GW), jnp.float32)
    for b in range(blocks):
        start = src_of(b) * (BLOCK * sub) + 2 * gl
        source = jnp.concatenate(
            [ext[pl.ds(start + c, WINDOW, stride=sub), :] for c in range(2)], axis=1
        )
        at = lax.broadcasted_iota(jnp.int32, (WINDOW, BLOCK), 0) - off_row(b)
        taps = jnp.zeros((WINDOW, BLOCK), jnp.float32)
        for t in range(TAPS):
            taps = jnp.where(at == t, weight_row(t, b), taps)
        t_hi, t_lo = split(taps)
        s_hi, s_lo = split(source)
        left = jnp.concatenate([t_hi, t_lo, t_hi], axis=0)
        right = jnp.concatenate([s_hi, s_hi, s_lo], axis=0)
        value = lax.dot_general(
            left, right, (((0,), (0,)), ((), ())), preferred_element_type=jnp.float32
        )
        for c in range(2):
            half = value[:, c * GW:(c + 1) * GW]
            out[pl.ds(b * BLOCK * sub + 2 * gl + c, BLOCK, stride=sub), :] = half
            energy = energy + jnp.sum((half * half).reshape(BLOCK // 8, 8, GW), axis=0)
    return energy


def remap_kernel(rows, blocks, chunk, per_chunk, halo_rows, src_ref, off_ref, w_ref, spec_ref, *rest):
    halos = rest[:len(halo_rows)]
    out_ref, energy_ref, ext, sems = rest[len(halo_rows):]
    sub = 2 * per_chunk
    copies = [pltpu.make_async_copy(
        spec_ref.at[:, pl.ds(chunk * sub, sub), :], ext.at[pl.ds(0, rows)], sems.at[0])]
    at = rows
    for i, count in enumerate(halo_rows):
        copies.append(pltpu.make_async_copy(halos[i], ext.at[pl.ds(at, count)], sems.at[i + 1]))
        at += count
    for copy in copies:
        copy.start()
    for copy in copies:
        copy.wait()
    flat = ext.reshape(ext.shape[0] * sub, GW)
    out = out_ref.reshape(rows * sub, GW)
    energy = jnp.zeros((8, GW), jnp.float32)
    for gl in range(per_chunk):
        g = chunk * per_chunk + gl
        energy = energy + remap_group(
            flat, out, sub, gl, blocks,
            lambda b: src_ref[g, b],
            lambda b: off_ref[pl.ds(g, 1), pl.ds(b * BLOCK, BLOCK)],
            lambda t, b: w_ref[t, pl.ds(g, 1), pl.ds(b * BLOCK, BLOCK)],
        )
    energy_ref[...] = energy


def remap_chunk(spec, halos, local_src, offsets, weights, chunk, per_chunk):
    rows = spec.shape[0]
    blocks = rows // BLOCK
    sub = 2 * per_chunk
    halo_rows = tuple(h.shape[0] for h in halos)
    vmem = pl.BlockSpec(memory_space=pltpu.VMEM)
    hbm = pl.BlockSpec(memory_space=pl.ANY)
    return pl.pallas_call(
        functools.partial(remap_kernel, rows, blocks, chunk, per_chunk, halo_rows),
        out_shape=(
            jax.ShapeDtypeStruct((rows, sub, GW), jnp.float32),
            jax.ShapeDtypeStruct((8, GW), jnp.float32),
        ),
        in_specs=[pl.BlockSpec(memory_space=pltpu.SMEM), vmem, vmem, hbm] + [hbm] * len(halos),
        out_specs=(vmem, vmem),
        scratch_shapes=[
            pltpu.VMEM((rows + sum(halo_rows), sub, GW), jnp.float32),
            pltpu.SemaphoreType.DMA((1 + len(halos),)),
        ],
        cost_estimate=pl.CostEstimate(flops=3_000_000_000, bytes_accessed=8_000_000, transcendentals=0),
    )(local_src, offsets, weights, spec, *halos)


def dft_kernel(rows, chunks, scale_ref, a_hi_ref, a_lo_ref, twist_ref, b_hi_ref, b_lo_ref, *rest):
    parts, out_ref = rest[:chunks], rest[chunks]
    total_groups = a_hi_ref.shape[0] // 2
    scale = scale_ref[0, 0]
    halves = total_groups // GW
    for r in range(rows):
        x = jnp.concatenate(
            [p[:, r].reshape(p.shape[0] * p.shape[2], GW) for p in parts], axis=0)
        x_hi, x_lo = split(x)
        both = jnp.dot(a_hi_ref[...], jnp.concatenate([x_hi, x_lo], axis=1), preferred_element_type=jnp.float32)
        y = both[:, :GW] + both[:, GW:] + jnp.dot(a_lo_ref[...], x_hi, preferred_element_type=jnp.float32)
        y_re, y_im = y[:total_groups], y[total_groups:]
        t_re, t_im = twist_ref[0], twist_ref[1]
        z = jnp.concatenate([y_re * t_re - y_im * t_im, y_re * t_im + y_im * t_re], axis=1)
        z_hi, z_lo = split(z * scale)
        nt = (((1,), (1,)), ((), ()))
        v = (
            lax.dot_general(b_hi_ref[...], z_hi, nt, preferred_element_type=jnp.float32)
            + lax.dot_general(b_hi_ref[...], z_lo, nt, preferred_element_type=jnp.float32)
            + lax.dot_general(b_lo_ref[...], z_hi, nt, preferred_element_type=jnp.float32)
        )
        for c in range(2):
            for h in range(halves):
                out_ref[r, pl.ds(2 * h + c, GW, stride=2 * halves), :] = (
                    v[c * GW:(c + 1) * GW, h * GW:(h + 1) * GW])


def inverse(parts, scale, tables):
    a_hi, a_lo, twist, b_hi, b_lo = tables
    az, rows, sub, _ = parts[0].shape
    step = min(rows, 4)
    whole = lambda shape: pl.BlockSpec(shape, lambda i: (0,) * len(shape))
    return pl.pallas_call(
        functools.partial(dft_kernel, step, len(parts)),
        out_shape=jax.ShapeDtypeStruct((rows, a_hi.shape[0], GW), jnp.float32),
        grid=(rows // step,),
        in_specs=[pl.BlockSpec(memory_space=pltpu.SMEM)]
        + [whole(t.shape) for t in tables]
        + [pl.BlockSpec((az, step, sub, GW), lambda i: (0, i, 0, 0))] * len(parts),
        out_specs=pl.BlockSpec((step, a_hi.shape[0], GW), lambda i: (i, 0, 0)),
        cost_estimate=pl.CostEstimate(flops=10_000_000_000, bytes_accessed=20_000_000, transcendentals=0),
    )(scale, *tables, *parts)


def halo_counts(rows_dev, rng_count):
    total = rows_dev * rng_count
    halo = min(rows_dev - BLOCK + SHIFT_B * BLOCK, total - 2 * BLOCK) + WINDOW - rows_dev
    counts = []
    distance = 1
    while halo > 0:
        counts.append(min(halo, rows_dev))
        halo -= rows_dev
        distance += 1
    return counts


def body(spectrum, src_block, offsets, tap_weights):
    rows_dev = spectrum.shape[0]
    columns = spectrum.shape[2]
    groups = columns // GW
    blocks_dev = rows_dev // BLOCK
    rng_count = lax.axis_size("rng")
    az_count = lax.axis_size("az")
    rows_after = rows_dev // az_count
    per_chunk = min(CHUNK_GROUPS, groups)
    chunks = groups // per_chunk
    sub = 2 * per_chunk
    total_len = columns * az_count
    total_cells = rows_dev * rng_count * total_len
    tables = dft_tables(az_count, groups, per_chunk)
    spec = spectrum.reshape(rows_dev, 2, groups, GW).transpose(0, 2, 1, 3).reshape(rows_dev, 2 * groups, GW)
    local_src = src_block - lax.axis_index("rng") * blocks_dev
    counts = halo_counts(rows_dev, rng_count)
    parts, energies = [], []
    for chunk in range(chunks):
        halos = []
        for i, count in enumerate(counts):
            pairs = [(p, p - i - 1) for p in range(rng_count) if p - i - 1 >= 0]
            piece = spec[:count, chunk * sub:(chunk + 1) * sub]
            halos.append(lax.ppermute(piece, "rng", pairs))
        part, energy = remap_chunk(spec, halos, local_src, offsets, tap_weights, chunk, per_chunk)
        energies.append(energy)
        parts.append(lax.all_to_all(
            part.reshape(az_count, rows_after, sub, GW), "az", split_axis=0, concat_axis=0, tiled=True))
    energy = lax.psum(jnp.sum(sum(energies)) / total_len, ("rng", "az"))
    scale = lax.rsqrt(energy / total_cells + 1e-06).reshape(1, 1)
    image = inverse(parts, scale, tables)
    return (
        image.reshape(rows_after, total_len // GW, 2, GW)
        .transpose(0, 2, 1, 3)
        .reshape(rows_after, 2, total_len)
    )


def solution(mesh):
    placed = (P("rng", None, "az"), P("az", "rng"), P("az", "rng"), P(None, "az", "rng"))
    return jax.shard_map(
        body, mesh=mesh, in_specs=placed, out_specs=P(("rng", "az"), None, None), check_vma=False
    )
```

```python
import functools
import math

import jax
import jax.numpy as jnp
import numpy as np
from jax import lax
from jax.experimental import pallas as pl
from jax.experimental.pallas import tpu as pltpu
from jax.sharding import PartitionSpec as P

BLOCK = 128
GW = 128
TAPS = 8
SHIFT_B = 5
WINDOW = 144
CHUNK_GROUPS = 4

MESH = pl.DeviceIdType.MESH


def split_np(x):
    hi = x.astype(jnp.bfloat16)
    lo = (x - hi.astype(np.float64)).astype(jnp.bfloat16)
    return hi, lo


def split(x):
    hi = x.astype(jnp.bfloat16)
    lo = (x - hi.astype(jnp.float32)).astype(jnp.bfloat16)
    return hi, lo


def dft_tables(az_count, groups, per_chunk):
    total_groups = az_count * groups
    chunks = groups // per_chunk
    total_len = total_groups * GW
    k1 = np.arange(total_groups)
    ch, az, gl = np.meshgrid(np.arange(chunks), np.arange(az_count), np.arange(per_chunk), indexing="ij")
    g = (az * groups + ch * per_chunk + gl).reshape(-1)
    angle = 2.0 * np.pi * ((k1[:, None] * g[None, :]) % total_groups) / total_groups
    first = np.empty((2, total_groups, g.size, 2))
    first[0, :, :, 0] = np.cos(angle)
    first[0, :, :, 1] = -np.sin(angle)
    first[1, :, :, 0] = np.sin(angle)
    first[1, :, :, 1] = np.cos(angle)
    first = first.reshape(2 * total_groups, 2 * total_groups)
    l = np.arange(GW)
    turn = 2.0 * np.pi * (k1[:, None] * l[None, :]) / total_len
    twist = np.stack([np.cos(turn), np.sin(turn)]).astype(np.float32) / np.float32(total_len)
    inner = 2.0 * np.pi * ((l[:, None] * l[None, :]) % GW) / GW
    second = np.empty((2, GW, 2, GW))
    second[0, :, 0] = np.cos(inner)
    second[0, :, 1] = -np.sin(inner)
    second[1, :, 0] = np.sin(inner)
    second[1, :, 1] = np.cos(inner)
    second = second.reshape(2 * GW, 2 * GW)
    a_hi, a_lo = split_np(first)
    b_hi, b_lo = split_np(second)
    return a_hi, a_lo, twist, b_hi, b_lo


def remap_group(ext, out, sub, gl, blocks, src_of, off_row, weight_row):
    energy = jnp.zeros((8, GW), jnp.float32)
    for b in range(blocks):
        start = src_of(b) * (BLOCK * sub) + 2 * gl
        source = jnp.concatenate(
            [ext[pl.ds(start + c, WINDOW, stride=sub), :] for c in range(2)], axis=1
        )
        at = lax.broadcasted_iota(jnp.int32, (WINDOW, BLOCK), 0) - off_row(b)
        taps = jnp.zeros((WINDOW, BLOCK), jnp.float32)
        for t in range(TAPS):
            taps = jnp.where(at == t, weight_row(t, b), taps)
        t_hi, t_lo = split(taps)
        s_hi, s_lo = split(source)
        left = jnp.concatenate([t_hi, t_lo, t_hi], axis=0)
        right = jnp.concatenate([s_hi, s_hi, s_lo], axis=0)
        value = lax.dot_general(
            left, right, (((0,), (0,)), ((), ())), preferred_element_type=jnp.float32
        )
        for c in range(2):
            half = value[:, c * GW:(c + 1) * GW]
            out[pl.ds(b * BLOCK * sub + 2 * gl + c, BLOCK, stride=sub), :] = half
            energy = energy + jnp.sum((half * half).reshape(BLOCK // 8, 8, GW), axis=0)
    return energy


def exchange_kernel(rows, blocks, chunks, per_chunk, counts, src_ref, off_ref, w_ref, spec_ref,
                    recv_ref, energy_ref, *scratch):
    ext, stage = scratch[:chunks], scratch[chunks:2 * chunks]
    (e_own, e_rng, e_sum, e_az, local_sem, halo_send, halo_recv,
     part_send, part_recv, e_send, e_recv) = scratch[2 * chunks:]
    rng_count, az_count = lax.axis_size("rng"), lax.axis_size("az")
    p, q = lax.axis_index("rng"), lax.axis_index("az")
    sub = 2 * per_chunk
    piece = rows // az_count
    half = max(az_count // 2, 1)
    side, place = q // half, q % half

    def local(c):
        return pltpu.make_async_copy(
            spec_ref.at[:, pl.ds(c * sub, sub), :], ext[c].at[pl.ds(0, rows)], local_sem.at[c])

    def halo(c, i):
        return pltpu.make_async_remote_copy(
            src_ref=spec_ref.at[pl.ds(0, counts[i]), pl.ds(c * sub, sub), :],
            dst_ref=ext[c].at[pl.ds(rows + sum(counts[:i]), counts[i])],
            send_sem=halo_send.at[c, i], recv_sem=halo_recv.at[c, i],
            device_id={"rng": (p + rng_count - i - 1) % rng_count}, device_id_type=MESH)

    reach = [i for i in range(len(counts)) if i + 1 < rng_count]
    for c in range(chunks):
        for i in reach:
            pl.when(p >= i + 1)(lambda c=c, i=i: halo(c, i).start())
        local(c).start()

    energy = jnp.zeros((8, GW), jnp.float32)
    for c in range(chunks):
        local(c).wait()
        for i in reach:
            pl.when(p + i + 1 < rng_count)(lambda c=c, i=i: halo(c, i).wait_recv())
        flat = ext[c].reshape(ext[c].shape[0] * sub, GW)
        out = stage[c].reshape(rows * sub, GW)
        for gl in range(per_chunk):
            g = c * per_chunk + gl
            energy = energy + remap_group(
                flat, out, sub, gl, blocks,
                lambda b: src_ref[g, b],
                lambda b: off_ref[pl.ds(g, 1), pl.ds(b * BLOCK, BLOCK)],
                lambda t, b: w_ref[t, pl.ds(g, 1), pl.ds(b * BLOCK, BLOCK)],
            )

        def send(peer, c=c):
            pltpu.make_async_remote_copy(
                src_ref=stage[c].at[pl.ds(peer * piece, piece)],
                dst_ref=recv_ref.at[c, q],
                send_sem=part_send.at[c], recv_sem=part_recv.at[c],
                device_id={"az": peer}, device_id_type=MESH).start()

        @pl.loop(0, half)
        def _(j):
            send((1 - side) * half + (place + j) % half)

        @pl.loop(1, half)
        def _(j):
            send(side * half + (place + j) % half)

        pltpu.make_async_copy(
            stage[c].at[pl.ds(q * piece, piece)], recv_ref.at[c, q], part_recv.at[c]).start()

    def share(src, dst, slot, axis, peer, stage_at):
        return pltpu.make_async_remote_copy(
            src_ref=src, dst_ref=dst.at[slot], send_sem=e_send.at[stage_at],
            recv_sem=e_recv.at[stage_at], device_id={axis: peer}, device_id_type=MESH)

    def spread(src, dst, slot, axis, count, stage_at):
        @pl.loop(1, count)
        def _(j):
            share(src, dst, slot, axis, (slot + j) % count, stage_at).start()
        others = dst.at[pl.ds(0, count - 1)]
        pltpu.make_async_copy(others, others, e_send.at[stage_at]).wait()
        pltpu.make_async_copy(others, others, e_recv.at[stage_at]).wait()

    e_own[...] = energy
    e_rng[p] = energy
    spread(e_own, e_rng, p, "rng", rng_count, 0)
    energy = jnp.sum(e_rng[...], axis=0)
    e_sum[...] = energy
    e_az[q] = energy
    spread(e_sum, e_az, q, "az", az_count, 1)
    energy_ref[...] = jnp.sum(e_az[...], axis=0)

    for c in range(chunks):
        pltpu.make_async_copy(recv_ref.at[c], recv_ref.at[c], part_recv.at[c]).wait()
        sent = stage[c].at[pl.ds(0, rows - piece)]
        pltpu.make_async_copy(sent, sent, part_send.at[c]).wait()
        for i in reach:
            pl.when(p >= i + 1)(lambda c=c, i=i: halo(c, i).wait_send())


def exchange(spec, local_src, offsets, weights, counts, per_chunk, rng_count, az_count):
    rows, width, _ = spec.shape
    blocks = rows // BLOCK
    sub = 2 * per_chunk
    chunks = width // sub
    piece = rows // az_count
    vmem = pl.BlockSpec(memory_space=pltpu.VMEM)
    hbm = pl.BlockSpec(memory_space=pl.ANY)
    tile = (8, GW)
    dma = pltpu.SemaphoreType.DMA
    return pl.pallas_call(
        functools.partial(exchange_kernel, rows, blocks, chunks, per_chunk, counts),
        out_shape=(
            jax.ShapeDtypeStruct((chunks, az_count, piece, sub, GW), jnp.float32),
            jax.ShapeDtypeStruct(tile, jnp.float32),
        ),
        in_specs=[pl.BlockSpec(memory_space=pltpu.SMEM), vmem, vmem, hbm],
        out_specs=(hbm, vmem),
        scratch_shapes=[pltpu.VMEM((rows + sum(counts), sub, GW), jnp.float32)] * chunks
        + [pltpu.VMEM((rows, sub, GW), jnp.float32)] * chunks
        + [
            pltpu.VMEM(tile, jnp.float32),
            pltpu.VMEM((rng_count,) + tile, jnp.float32),
            pltpu.VMEM(tile, jnp.float32),
            pltpu.VMEM((az_count,) + tile, jnp.float32),
            dma((chunks,)),
            dma((chunks, len(counts))),
            dma((chunks, len(counts))),
            dma((chunks,)),
            dma((chunks,)),
            dma((2,)),
            dma((2,)),
        ],
        compiler_params=pltpu.CompilerParams(has_side_effects=True, vmem_limit_bytes=60 * 1024 * 1024),
    )(local_src, offsets, weights, spec)


def dft_kernel(rows, chunks, scale_ref, a_hi_ref, a_lo_ref, twist_ref, b_hi_ref, b_lo_ref, *rest):
    parts_ref, out_ref = rest
    total_groups = a_hi_ref.shape[0] // 2
    scale = scale_ref[0, 0]
    halves = total_groups // GW
    for r in range(rows):
        x = jnp.concatenate(
            [parts_ref[c, :, r].reshape(2 * total_groups // chunks, GW) for c in range(chunks)], axis=0)
        x_hi, x_lo = split(x)
        both = jnp.dot(a_hi_ref[...], jnp.concatenate([x_hi, x_lo], axis=1), preferred_element_type=jnp.float32)
        y = both[:, :GW] + both[:, GW:] + jnp.dot(a_lo_ref[...], x_hi, preferred_element_type=jnp.float32)
        y_re, y_im = y[:total_groups], y[total_groups:]
        t_re, t_im = twist_ref[0], twist_ref[1]
        z = jnp.concatenate([y_re * t_re - y_im * t_im, y_re * t_im + y_im * t_re], axis=1)
        z_hi, z_lo = split(z * scale)
        nt = (((1,), (1,)), ((), ()))
        v = (
            lax.dot_general(b_hi_ref[...], z_hi, nt, preferred_element_type=jnp.float32)
            + lax.dot_general(b_hi_ref[...], z_lo, nt, preferred_element_type=jnp.float32)
            + lax.dot_general(b_lo_ref[...], z_hi, nt, preferred_element_type=jnp.float32)
        )
        for c in range(2):
            for h in range(halves):
                out_ref[r, pl.ds(2 * h + c, GW, stride=2 * halves), :] = (
                    v[c * GW:(c + 1) * GW, h * GW:(h + 1) * GW])


def inverse(parts, scale, tables):
    a_hi, a_lo, twist, b_hi, b_lo = tables
    chunks, az, rows, sub, _ = parts.shape
    step = min(rows, 4)
    whole = lambda shape: pl.BlockSpec(shape, lambda i: (0,) * len(shape))
    return pl.pallas_call(
        functools.partial(dft_kernel, step, chunks),
        out_shape=jax.ShapeDtypeStruct((rows, a_hi.shape[0], GW), jnp.float32),
        grid=(rows // step,),
        in_specs=[pl.BlockSpec(memory_space=pltpu.SMEM)]
        + [whole(t.shape) for t in tables]
        + [pl.BlockSpec((chunks, az, step, sub, GW), lambda i: (0, 0, i, 0, 0))],
        out_specs=pl.BlockSpec((step, a_hi.shape[0], GW), lambda i: (i, 0, 0)),
        cost_estimate=pl.CostEstimate(flops=10_000_000_000, bytes_accessed=20_000_000, transcendentals=0),
    )(scale, *tables, parts)


def halo_counts(rows_dev, rng_count):
    total = rows_dev * rng_count
    halo = min(rows_dev - BLOCK + SHIFT_B * BLOCK, total - 2 * BLOCK) + WINDOW - rows_dev
    counts = []
    distance = 1
    while halo > 0:
        counts.append(min(halo, rows_dev))
        halo -= rows_dev
        distance += 1
    return counts


def body(spectrum, src_block, offsets, tap_weights):
    rows_dev = spectrum.shape[0]
    columns = spectrum.shape[2]
    groups = columns // GW
    blocks_dev = rows_dev // BLOCK
    rng_count = lax.axis_size("rng")
    az_count = lax.axis_size("az")
    rows_after = rows_dev // az_count
    per_chunk = min(CHUNK_GROUPS, groups)
    total_len = columns * az_count
    total_cells = rows_dev * rng_count * total_len
    tables = dft_tables(az_count, groups, per_chunk)
    spec = spectrum.reshape(rows_dev, 2, groups, GW).transpose(0, 2, 1, 3).reshape(rows_dev, 2 * groups, GW)
    local_src = src_block - lax.axis_index("rng") * blocks_dev
    counts = halo_counts(rows_dev, rng_count)
    parts, energies = exchange(
        spec, local_src, offsets, tap_weights, counts, per_chunk, rng_count, az_count)
    energy = jnp.sum(energies) / total_len
    scale = lax.rsqrt(energy / total_cells + 1e-06).reshape(1, 1)
    image = inverse(parts, scale, tables)
    return (
        image.reshape(rows_after, total_len // GW, 2, GW)
        .transpose(0, 2, 1, 3)
        .reshape(rows_after, 2, total_len)
    )


def solution(mesh):
    placed = (P("rng", None, "az"), P("az", "rng"), P("az", "rng"), P(None, "az", "rng"))
    return jax.shard_map(
        body, mesh=mesh, in_specs=placed, out_specs=P(("rng", "az"), None, None), check_vma=False
    )
```
